768 devices in a mesh: dom: 768 (over z, x, y, core).
Axes of the slice: x: 4, y: 8, z: 12, core: 2. Of those that a mesh axis runs over, the one named last changes fastest.
Arguments:
- states: float32 [393216, 128], P('dom'), may hold values from -6 to 6
- diag_blocks: float32 [3072, 128, 128], P('dom'), may hold values from -0.5 to 0.5
- couplings: float32 [3072, 128, 128], P('dom'), may hold values from -0.5 to 0.5
Outputs:
- orthonormal: float32 [393216, 128], P('dom')
- projected: float32 [128, 128], replicated
The draws below stay inside these ranges and needn't reach their ends.
All inputs are finite; a program needn't handle non-finite values.
Results may differ from the reference program's by a relative error of at most 0.00012.
Values sent between devices are 32-bit elements; how exact they have to be, the bound alone decides.
A program may use at most 32 MiB of HBM per device.

```python
import math
import jax
import jax.numpy as jnp
from jax import lax

NB = 128
BLOCK = 128
NODES = 393216
BLOCKS = 3072


def block_levels(own_key, dims, pieces, least, largest):
    def one(position, shards_of):
        steps = jax.random.uniform(jax.random.fold_in(jax.random.fold_in(own_key, 6), position), (shards_of,), jnp.float32, least / len(pieces), largest / len(pieces))
        return jnp.repeat(jnp.exp(steps), dims[position] // shards_of).reshape((-1,) + (1,) * (len(dims) - position - 1))

    gain = one(*pieces[0])
    for cut in pieces[1:]:
        gain = gain * one(*cut)
    return gain


def noise(key, shape, spread, reach, shards=(), kind=jnp.bfloat16):
    loudness = block_levels(key, shape, shards, -0.22, 0.18) if shards else 1.0
    values = jax.random.normal(key, shape, jnp.float32) * spread * loudness
    return jnp.minimum(jnp.maximum(values, -reach), reach).astype(kind)


def setup_inputs(seed: int = 0) -> dict:
    seeds = jax.random.split(jax.random.key(seed), 4)
    return {
        "states": noise(seeds[0], (NODES, NB), 1.0, 6.0, ((0, 768),), jnp.float32),
        "diag_blocks": noise(seeds[1], (BLOCKS, BLOCK, BLOCK), BLOCK ** -0.5, 0.5, ((0, 768),), jnp.float32),
        "couplings": noise(seeds[2], (BLOCKS, BLOCK, BLOCK), BLOCK ** -0.5, 0.5, ((0, 768),), jnp.float32),
    }


center = 0.5
half_width = 4.0

def lower_solve(factor, values):
    return lax.linalg.triangular_solve(factor, values, left_side=True, lower=True)

def apply_band(extended, diag_ext, coup_ext):
    inside = jnp.einsum('bij,bjs->bis', diag_ext[1:-1], extended[1:-1], precision=lax.Precision.HIGHEST)
    upward = jnp.einsum('bij,bjs->bis', coup_ext[1:-1], extended[2:], precision=lax.Precision.HIGHEST)
    downward = jnp.einsum('bji,bjs->bis', coup_ext[:-2], extended[:-2], precision=lax.Precision.HIGHEST)
    return inside + upward + downward

def pad_blocks(values):
    return jnp.pad(values, ((1, 1), (0, 0), (0, 0)))

def reference(states, diag_blocks, couplings):
    symmetric = 0.5 * (diag_blocks + jnp.swapaxes(diag_blocks, 1, 2))
    diag_ext = pad_blocks(symmetric)
    coup_ext = pad_blocks(couplings)
    field = states.reshape(BLOCKS, BLOCK, NB)
    first = (apply_band(pad_blocks(field), diag_ext, coup_ext) - center * field) / half_width
    filtered = 2.0 * (apply_band(pad_blocks(first), diag_ext, coup_ext) - center * first) / half_width - field
    image = apply_band(pad_blocks(filtered), diag_ext, coup_ext)
    flat = filtered.reshape(NODES, NB)
    correlation = jnp.einsum('ns,nt->st', flat, flat, precision=lax.Precision.HIGHEST)
    mixed = jnp.einsum('ns,nt->st', flat, image.reshape(NODES, NB), precision=lax.Precision.HIGHEST)
    lower = jnp.linalg.cholesky(correlation)
    orthonormal = lower_solve(lower, flat.T).T * math.sqrt(NODES)
    left = lower_solve(lower, mixed)
    projected = lower_solve(lower, left.T).T
    return (orthonormal, projected)
```

```python
import functools
import math

import jax
import jax.numpy as jnp
from jax import lax
from jax.experimental import pallas as pl
from jax.experimental.pallas import tpu as pltpu
from jax.sharding import Mesh
from jax.sharding import PartitionSpec as P

DOM = ("dom_0", "dom_1", "dom_2", "dom_3")
NZ, NX, NY, NC = 12, 4, 8, 2
PLANE = NX * NY * NC
PIECES = 17
MESH = pl.DeviceIdType.MESH

center = 0.5
half_width = 4.0


def with_halo(block, sides, width):
    for axis, dim in sides:
        count = lax.axis_size(axis)
        forward = [(i, i + 1) for i in range(count - 1)]
        backward = [(target, source) for source, target in forward]
        low = lax.ppermute(
            lax.slice_in_dim(block, block.shape[dim] - width, None, axis=dim), axis, forward
        )
        high = lax.ppermute(lax.slice_in_dim(block, 0, width, axis=dim), axis, backward)
        block = jnp.concatenate([low, block, high], axis=dim)
    return block


def lower_solve(factor, values):
    return lax.linalg.triangular_solve(factor, values, left_side=True, lower=True)


def apply_band(extended, diag_ext, coup_ext):
    inside = jnp.einsum(
        "bij,bjs->bis", diag_ext[1:-1], extended[1:-1], precision=lax.Precision.HIGHEST
    )
    upward = jnp.einsum(
        "bij,bjs->bis", coup_ext[1:-1], extended[2:], precision=lax.Precision.HIGHEST
    )
    downward = jnp.einsum(
        "bji,bjs->bis", coup_ext[:-2], extended[:-2], precision=lax.Precision.HIGHEST
    )
    return inside + upward + downward


def gram_matrix(left, right):
    return jnp.einsum("ns,nt->st", left, right, precision=lax.Precision.HIGHEST)


def owner_of(piece):
    ox = jnp.where(piece < 16, piece // 4, 0)
    oy = jnp.where(piece < 16, 2 * (piece % 4) + ox % 2, 1)
    return ox, oy


def reduce_kernel(x_ref, o_ref, recv1, recv2, recv3, send1, rsem1, send2, rsem2, send3, rsem3):
    z, x, y, c = (lax.axis_index(a) for a in DOM)
    me = (x * NY + y) * NC + c
    even = (x + y) % 2 == 0
    owner = jnp.logical_and(c == 1, jnp.logical_or(even, jnp.logical_and(x == 0, y == 1)))
    mine = jnp.where(even, x * 4 + y // 2, 16)

    def plane_id(t):
        return (z, t // (NY * NC), (t // NC) % NY, t % NC)

    barrier = pltpu.get_barrier_semaphore()

    @pl.when(owner)
    def _():
        def to_plane(r, carry):
            pl.semaphore_signal(barrier, inc=1, device_id=plane_id((me + r) % PLANE), device_id_type=MESH)
            return carry

        lax.fori_loop(1, PLANE, to_plane, 0)

        def to_column(r, carry):
            pl.semaphore_signal(barrier, inc=1, device_id=((z + r) % NZ, x, y, c), device_id_type=MESH)
            return carry

        lax.fori_loop(1, NZ, to_column, 0)
        pl.semaphore_wait(barrier, PLANE - 1 + NZ - 1)

    @pl.when(jnp.logical_not(owner))
    def _():
        def to_owner(r, carry):
            ox, oy = owner_of(r)
            pl.semaphore_signal(barrier, inc=1, device_id=(z, ox, oy, 1), device_id_type=MESH)
            return carry

        lax.fori_loop(0, PIECES, to_owner, 0)
        pl.semaphore_wait(barrier, PIECES)

    def scatter(r, carry):
        piece = (r + me) % PIECES
        ox, oy = owner_of(piece)
        target = (ox * NY + oy) * NC + 1

        @pl.when(target == me)
        def _():
            recv1[0] = x_ref[piece]

        @pl.when(target != me)
        def _():
            pltpu.make_async_remote_copy(
                src_ref=x_ref.at[piece],
                dst_ref=recv1.at[(me - target + PLANE) % PLANE],
                send_sem=send1,
                recv_sem=rsem1,
                device_id=(z, ox, oy, 1),
                device_id_type=MESH,
            ).start()

        return carry

    lax.fori_loop(0, PIECES, scatter, 0)

    def arrived(ref, sem):
        pltpu.make_async_copy(ref, ref, sem).wait()

    @pl.when(owner)
    def _():
        arrived(recv1.at[pl.ds(1, PLANE - 1)], rsem1)
        recv2[z] = jnp.sum(recv1[...], axis=0)

        def exchange(r, carry):
            pltpu.make_async_remote_copy(
                src_ref=recv2.at[z],
                dst_ref=recv2.at[z],
                send_sem=send2,
                recv_sem=rsem2,
                device_id=((z + r) % NZ, x, y, c),
                device_id_type=MESH,
            ).start()
            return carry

        lax.fori_loop(1, NZ, exchange, 0)
        arrived(recv2.at[pl.ds(0, NZ - 1)], rsem2)
        recv3[mine] = jnp.sum(recv2[...], axis=0)

        def spread(r, carry):
            pltpu.make_async_remote_copy(
                src_ref=recv3.at[mine],
                dst_ref=recv3.at[mine],
                send_sem=send3,
                recv_sem=rsem3,
                device_id=plane_id((me + r) % PLANE),
                device_id_type=MESH,
            ).start()
            return carry

        lax.fori_loop(1, PLANE, spread, 0)
        arrived(recv3.at[pl.ds(0, PIECES - 1)], rsem3)
        arrived(recv1.at[pl.ds(0, PIECES - 1)], send1)
        arrived(recv2.at[pl.ds(0, NZ - 1)], send2)
        arrived(recv1.at[pl.ds(0, PLANE - 1)], send3)

    @pl.when(jnp.logical_not(owner))
    def _():
        arrived(recv3.at[pl.ds(0, PIECES)], rsem3)
        arrived(recv1.at[pl.ds(0, PIECES)], send1)

    o_ref[...] = recv3[...]


def all_reduce(packed):
    shape = (PIECES, 8, 128)
    return pl.pallas_call(
        reduce_kernel,
        out_shape=jax.ShapeDtypeStruct(shape, jnp.float32),
        in_specs=[pl.BlockSpec(memory_space=pltpu.VMEM)],
        out_specs=pl.BlockSpec(memory_space=pltpu.VMEM),
        scratch_shapes=[
            pltpu.VMEM((PLANE, 8, 128), jnp.float32),
            pltpu.VMEM((NZ, 8, 128), jnp.float32),
            pltpu.VMEM(shape, jnp.float32),
        ]
        + [pltpu.SemaphoreType.DMA(())] * 6,
        compiler_params=pltpu.CompilerParams(collective_id=0, has_side_effects=True),
    )(packed)


def body(states, diag_blocks, couplings):
    nodes_dev, width = states.shape
    nblocks, block, unused_width = diag_blocks.shape
    devices = lax.axis_size(DOM)
    total_nodes = nodes_dev * devices
    symmetric = 0.5 * (diag_blocks + jnp.swapaxes(diag_blocks, 1, 2))
    field = states.reshape(nblocks, block, width)
    stacked = jnp.stack([symmetric, couplings], 1)
    operator = with_halo(stacked, ((DOM, 0),), 2)
    extended = with_halo(field, ((DOM, 0),), 2)
    first = (
        apply_band(extended, operator[:, 0], operator[:, 1]) - center * extended[1:-1]
    ) / half_width
    position = lax.axis_index(DOM) * nblocks - 1 + jnp.arange(nblocks + 2, dtype=jnp.int32)
    inside_chain = (position >= 0) & (position < nblocks * devices)
    first = jnp.where(inside_chain[:, None, None], first, 0.0)
    diag_ext = operator[1:-1, 0]
    coup_ext = operator[1:-1, 1]
    filtered = (
        2.0 * (apply_band(first, diag_ext, coup_ext) - center * first[1:-1]) / half_width - field
    )
    flat = filtered.reshape(nodes_dev, width)
    extended = with_halo(filtered, ((DOM, 0),), 1)
    image = apply_band(extended, diag_ext, coup_ext).reshape(nodes_dev, width)
    own = gram_matrix(flat, flat)
    cross = gram_matrix(flat, image)
    cross = 0.5 * (cross + cross.T)
    rows = lax.broadcasted_iota(jnp.int32, (128, 128), 0)
    cols = lax.broadcasted_iota(jnp.int32, (128, 128), 1)
    packed = jnp.where(rows >= cols, own, cross)
    diagonal = jnp.sum(jnp.where(rows == cols, cross, 0.0), axis=0, keepdims=True)
    packed = jnp.concatenate([packed, jnp.pad(diagonal, ((0, 7), (0, 0)))], axis=0)
    total = all_reduce(packed.reshape(PIECES, 8, 128)).reshape(PIECES * 8, 128)
    square, diagonal = total[:128], total[128:129]
    correlation = jnp.where(rows >= cols, square, square.T)
    mixed = jnp.where(rows < cols, square, square.T)
    mixed = jnp.where(rows == cols, diagonal, mixed)
    lower = jnp.linalg.cholesky(correlation)
    orthonormal = lower_solve(lower, flat.T).T * math.sqrt(total_nodes)
    left = lower_solve(lower, mixed)
    projected = lower_solve(lower, left.T).T
    return (orthonormal, projected)


def solution(mesh):
    split = Mesh(mesh.devices.reshape(NZ, NX, NY, NC), DOM)
    in_specs = (P(DOM, None), P(DOM, None, None), P(DOM, None, None))
    out_specs = (P(DOM, None), P())
    return jax.shard_map(body, mesh=split, in_specs=in_specs, out_specs=out_specs, check_vma=False)
```

```python
import functools
import math

import jax
import jax.numpy as jnp
from jax import lax
from jax.experimental import pallas as pl
from jax.experimental.pallas import tpu as pltpu
from jax.sharding import Mesh
from jax.sharding import PartitionSpec as P

DOM = ("dom_0", "dom_1", "dom_2", "dom_3")
NZ, NX, NY, NC = 12, 4, 8, 2
PLANE = NX * NY * NC
PIECES = 17
MESH = pl.DeviceIdType.MESH

center = 0.5
half_width = 4.0

BS = 32
bf16 = jnp.bfloat16
f32 = jnp.float32


def split2(v):
    hi = v.astype(bf16)
    return hi, (v - hi.astype(f32)).astype(bf16)


def split3(v):
    hi = v.astype(bf16)
    rest = v - hi.astype(f32)
    mid = rest.astype(bf16)
    return hi, mid, (rest - mid.astype(f32)).astype(bf16)


def dot(a, b, ca=1, cb=0):
    return lax.dot_general(a, b, (((ca,), (cb,)), ((), ())), preferred_element_type=f32)


def dot6(a, b, ca=1, cb=0):
    (ah, am, al), (bh, bm, bl) = split3(a), split3(b)
    left = jnp.concatenate([ah, ah, am, am, ah, al], axis=ca)
    right = jnp.concatenate([bh, bm, bh, bm, bl, bh], axis=cb)
    return dot(left, right, ca, cb)


def dot3(a, b, ca=1, cb=0):
    (ah, al), (bh, bl) = split2(a), split2(b)
    return dot(ah, bh, ca, cb) + (dot(ah, bl, ca, cb) + dot(al, bh, ca, cb))


def spread_row(tile, s, width):
    return jnp.broadcast_to(tile[s : s + 1, :], (8, width))


def inverse_factor(a_ref, r_ref):
    n = 128
    tiles = BS // 8
    rows8 = lax.broadcasted_iota(jnp.int32, (8, 128), 0)
    for block in range(n // BS):
        base = block * BS
        square = a_ref[pl.ds(base, BS), :]
        cols = {}
        for j in range(BS):
            for r in range(j // 8, tiles):
                cols[j, r] = jnp.broadcast_to(
                    square[8 * r : 8 * r + 8, base + j : base + j + 1], (8, 128)
                )
        pa = [square[8 * r : 8 * r + 8, :] for r in range(tiles)]
        pr = [r_ref[pl.ds(base + 8 * r, 8), :] for r in range(tiles)]
        for k in range(BS):
            rk, sk = k // 8, k % 8
            inv = lax.rsqrt(spread_row(cols[k, rk], sk, 128))
            low = {r: cols[k, r] * inv for r in range(rk, tiles)}
            for j in range(k + 1, BS):
                factor = spread_row(low[j // 8], j % 8, 128)
                for r in range(j // 8, tiles):
                    cols[j, r] = cols[j, r] - low[r] * factor
            row_a = spread_row(pa[rk], sk, 128) * inv
            row_r = spread_row(pr[rk], sk, 128) * inv
            for r in range(rk, tiles):
                scale = low[r]
                if r == rk:
                    scale = jnp.where(rows8 > sk, scale, 0.0)
                na, nr = pa[r] - scale * row_a, pr[r] - scale * row_r
                if r == rk:
                    na, nr = jnp.where(rows8 == sk, row_a, na), jnp.where(rows8 == sk, row_r, nr)
                pa[r], pr[r] = na, nr
        upper = jnp.concatenate(pa, axis=0)
        below = jnp.concatenate(pr, axis=0)
        r_ref[pl.ds(base, BS), :] = below
        rest = n - base - BS
        if rest:
            both = jnp.concatenate([upper, below], axis=1)
            h, m, l = split3(both)
            lhs = jnp.concatenate([h, h, m, m, h, l], axis=0)[:, :128]
            rhs = jnp.concatenate([h, m, h, m, l, h], axis=0)
            update = dot(lhs, rhs, 0, 0)
            start = base + BS
            a_ref[pl.ds(start, rest), :] = a_ref[pl.ds(start, rest), :] - update[start:, :128]
            r_ref[pl.ds(start, rest), :] = r_ref[pl.ds(start, rest), :] - update[start:, 128:]


def finish_kernel(total_nodes, g_ref, f_ref, o_ref, p_ref, f_vmem, a_ref, r_ref, sem):
    load = pltpu.make_async_copy(f_ref, f_vmem, sem)
    load.start()
    rows = lax.broadcasted_iota(jnp.int32, (128, 128), 0)
    cols = lax.broadcasted_iota(jnp.int32, (128, 128), 1)
    square = g_ref[pl.ds(0, 128), :]
    diagonal = g_ref[pl.ds(128, 1), :]
    turned = square.T
    a_ref[...] = jnp.where(rows >= cols, square, turned)
    mixed = jnp.where(rows < cols, square, turned)
    mixed = jnp.where(rows == cols, jnp.broadcast_to(diagonal, (128, 128)), mixed)
    r_ref[...] = jnp.where(rows == cols, 1.0, 0.0)
    inverse_factor(a_ref, r_ref)
    inv = r_ref[...]
    p_ref[...] = dot6(dot6(inv, mixed), inv, 1, 1)
    load.wait()
    o_ref[...] = dot3(f_vmem[...], inv * math.sqrt(total_nodes), 1, 1)


def finish(packed, flat, total_nodes):
    n = flat.shape[0]
    return pl.pallas_call(
        functools.partial(finish_kernel, total_nodes),
        out_shape=(jax.ShapeDtypeStruct((n, 128), f32), jax.ShapeDtypeStruct((128, 128), f32)),
        in_specs=[pl.BlockSpec(memory_space=pltpu.VMEM), pl.BlockSpec(memory_space=pl.ANY)],
        out_specs=(pl.BlockSpec(memory_space=pltpu.VMEM),) * 2,
        scratch_shapes=[
            pltpu.VMEM((n, 128), f32),
            pltpu.VMEM((128, 128), f32),
            pltpu.VMEM((128, 128), f32),
            pltpu.SemaphoreType.DMA(()),
        ],
    )(packed, flat)


def halves(v):
    hi = v.astype(bf16)
    return hi, (v - hi.astype(f32)).astype(bf16)


def mul(a, b):
    (ah, al), (bh, bl) = a, b
    return dot(ah, bh) + (dot(ah, bl) + dot(al, bh))


def flip(pair):
    return tuple(part.T for part in pair)


def owner_of(piece):
    ox = jnp.where(piece < 16, piece // 4, 0)
    oy = jnp.where(piece < 16, 2 * (piece % 4) + ox % 2, 1)
    return ox, oy


def filter_kernel(
    s_ref, d_ref, c_ref, f_ref, o_ref,
    s, d, cp, out_left, out_right, from_right, from_left, flat, pieces,
    recv1, recv2, recv3,
    load_sem, store_sem, left_send, right_send, right_sem, left_sem,
    send1, rsem1, send2, rsem2, send3, rsem3,
):
    z, x, y, c = (lax.axis_index(a) for a in DOM)
    me = (x * NY + y) * NC + c
    lin = z * PLANE + me
    has_left = lin > 0
    has_right = lin < NZ * PLANE - 1
    even = (x + y) % 2 == 0
    owner = jnp.logical_and(c == 1, jnp.logical_or(even, jnp.logical_and(x == 0, y == 1)))
    mine = jnp.where(even, x * 4 + y // 2, 16)

    loads = [
        pltpu.make_async_copy(src, dst, load_sem.at[i])
        for i, (src, dst) in enumerate(((s_ref, s), (d_ref, d), (c_ref, cp)))
    ]
    for load in loads:
        load.start()

    def plane_id(t):
        return (z, t // (NY * NC), (t // NC) % NY, t % NC)

    def chain_id(t):
        return (t // PLANE, (t // (NY * NC)) % NX, (t // NC) % NY, t % NC)

    barrier = pltpu.get_barrier_semaphore()

    def greet(target):
        pl.semaphore_signal(barrier, inc=1, device_id=target, device_id_type=MESH)

    @pl.when(has_left)
    def _():
        greet(chain_id(lin - 1))

    @pl.when(has_right)
    def _():
        greet(chain_id(lin + 1))

    @pl.when(owner)
    def _():
        def to_plane(r, carry):
            greet(plane_id((me + r) % PLANE))
            return carry

        lax.fori_loop(1, PLANE, to_plane, 0)

        def to_column(r, carry):
            greet(((z + r) % NZ, x, y, c))
            return carry

        lax.fori_loop(1, NZ, to_column, 0)

    @pl.when(jnp.logical_not(owner))
    def _():
        def to_owner(r, carry):
            ox, oy = owner_of(r)
            greet((z, ox, oy, 1))
            return carry

        lax.fori_loop(0, PIECES, to_owner, 0)

    def arrived(ref, sem):
        pltpu.make_async_copy(ref, ref, sem).wait()

    for load in loads:
        load.wait()

    rows = lax.broadcasted_iota(jnp.int32, (128, 128), 0)
    cols = lax.broadcasted_iota(jnp.int32, (128, 128), 1)
    eye = rows == cols

    def shifted(raw):
        return halves(0.5 * (raw + raw.T) - jnp.where(eye, center, 0.0))

    def block(ref, b):
        return ref[pl.ds(128 * b, 128), :]

    quarter, half = 1.0 / half_width, 2.0 / half_width
    sv = [block(s, b) for b in range(4)]
    ss = [halves(v) for v in sv]
    cc = [halves(cp[b]) for b in range(4)]
    ct = [flip(v) for v in cc]
    aa = [shifted(d[b]) for b in range(4)]
    p0 = (mul(aa[0], ss[0]) + mul(cc[0], ss[1])) * quarter
    u = mul(ct[3], ss[3]) * quarter
    out_left[0] = p0
    out_right[0] = u
    g1 = (mul(aa[1], ss[1]) + mul(cc[1], ss[2]) + mul(ct[0], ss[0])) * quarter
    h3 = (mul(aa[3], ss[3]) + mul(ct[2], ss[2])) * quarter
    p0s, g1s, h3s, us = halves(p0), halves(g1), halves(h3), halves(u)
    q0 = (mul(aa[0], p0s) + mul(cc[0], g1s)) * half - sv[0]
    w = mul(ct[3], h3s) * half
    out_left[1] = q0
    out_right[1] = w

    greeted = has_left.astype(jnp.int32) + has_right.astype(jnp.int32)
    pl.semaphore_wait(barrier, jnp.where(owner, PLANE - 1 + NZ - 1, PIECES) + greeted)

    @pl.when(has_left)
    def _():
        for i, src in enumerate((s.at[pl.ds(0, 128)], d.at[0], out_left.at[0], out_left.at[1])):
            pltpu.make_async_remote_copy(
                src_ref=src, dst_ref=from_right.at[i], send_sem=left_send, recv_sem=right_sem.at[i],
                device_id=chain_id(lin - 1), device_id_type=MESH,
            ).start()

    @pl.when(has_right)
    def _():
        for i, src in enumerate((cp.at[3], out_right.at[0], out_right.at[1])):
            pltpu.make_async_remote_copy(
                src_ref=src, dst_ref=from_left.at[i], send_sem=right_send, recv_sem=left_sem.at[i],
                device_id=chain_id(lin + 1), device_id_type=MESH,
            ).start()

    @pl.when(jnp.logical_not(has_right))
    def _():
        from_right[...] = jnp.zeros_like(from_right)

    @pl.when(jnp.logical_not(has_left))
    def _():
        from_left[...] = jnp.zeros_like(from_left)

    g2 = (mul(aa[2], ss[2]) + mul(cc[2], ss[3]) + mul(ct[1], ss[1])) * quarter
    g2s = halves(g2)
    e1 = (mul(aa[1], g1s) + mul(ct[0], p0s) + mul(cc[1], g2s)) * half - sv[1]
    e2 = (mul(aa[2], g2s) + mul(ct[1], g1s) + mul(cc[2], h3s)) * half - sv[2]
    e3 = (mul(aa[3], h3s) + mul(ct[2], g2s)) * half - sv[3]

    @pl.when(has_right)
    def _():
        for i in range(4):
            arrived(from_right.at[i], right_sem.at[i])

    @pl.when(has_left)
    def _():
        for i in range(3):
            arrived(from_left.at[i], left_sem.at[i])

    inside = jnp.where(has_right, 1.0, 0.0)
    v = mul(cc[3], halves(from_right[0])) * quarter
    vs = halves(v)
    g3s = halves(h3 + v)
    g4s = halves((from_right[2] + u) * inside)
    cl = halves(from_left[0])
    ul = halves(from_left[1])
    back = mul(flip(cl), halves(mul(cl, ss[0])))
    f4 = (from_right[3] + (mul(shifted(from_right[1]), us) + mul(ct[3], g3s)) * half) * inside
    f0 = q0 + mul(aa[0], ul) * half + from_left[2] + back * (half * quarter)
    f1 = e1 + mul(ct[0], ul) * half
    f2 = e2 + mul(cc[2], vs) * half
    f3 = e3 + (mul(aa[3], vs) + mul(cc[3], g4s)) * half
    fs = [f0, f1, f2, f3, f4]
    for b in range(4):
        flat[pl.ds(128 * b, 128), :] = fs[b]
    store = pltpu.make_async_copy(flat, f_ref, store_sem)
    store.start()
    fh = [halves(f) for f in fs]
    part = [mul(halves(0.5 * d[b]), fh[b]) + mul(cc[b], fh[b + 1]) for b in range(4)]
    ph = [halves(g) for g in part]
    th = jnp.concatenate([h for h, l in fh[:4]], axis=0).T
    tl = jnp.concatenate([l for h, l in fh[:4]], axis=0).T
    wh = jnp.concatenate([jnp.concatenate([fh[b][0], ph[b][0]], axis=1) for b in range(4)], axis=0)
    wl = jnp.concatenate([jnp.concatenate([fh[b][1], ph[b][1]], axis=1) for b in range(4)], axis=0)
    both = dot(th, wh) + (dot(th, wl) + dot(tl, wh))
    own, cross = both[:, :128], both[:, 128:]
    cross = cross + cross.T
    packed = jnp.where(rows >= cols, own, cross)
    diagonal = jnp.sum(jnp.where(eye, cross, 0.0), axis=0, keepdims=True)
    for i in range(16):
        pieces[i] = packed[8 * i : 8 * i + 8, :]
    pieces[16] = jnp.where(lax.broadcasted_iota(jnp.int32, (8, 128), 0) == 0, diagonal, 0.0)

    def scatter(r, carry):
        piece = (r + me) % PIECES
        ox, oy = owner_of(piece)
        target = (ox * NY + oy) * NC + 1

        @pl.when(target == me)
        def _():
            recv1[0] = pieces[piece]

        @pl.when(target != me)
        def _():
            pltpu.make_async_remote_copy(
                src_ref=pieces.at[piece],
                dst_ref=recv1.at[(me - target + PLANE) % PLANE],
                send_sem=send1,
                recv_sem=rsem1,
                device_id=(z, ox, oy, 1),
                device_id_type=MESH,
            ).start()

        return carry

    lax.fori_loop(0, PIECES, scatter, 0)

    @pl.when(owner)
    def _():
        arrived(recv1.at[pl.ds(1, PLANE - 1)], rsem1)
        recv2[z] = jnp.sum(recv1[...], axis=0)

        def exchange(r, carry):
            pltpu.make_async_remote_copy(
                src_ref=recv2.at[z],
                dst_ref=recv2.at[z],
                send_sem=send2,
                recv_sem=rsem2,
                device_id=((z + r) % NZ, x, y, c),
                device_id_type=MESH,
            ).start()
            return carry

        lax.fori_loop(1, NZ, exchange, 0)
        arrived(recv2.at[pl.ds(0, NZ - 1)], rsem2)
        recv3[mine] = jnp.sum(recv2[...], axis=0)

        def spread(r, carry):
            pltpu.make_async_remote_copy(
                src_ref=recv3.at[mine],
                dst_ref=recv3.at[mine],
                send_sem=send3,
                recv_sem=rsem3,
                device_id=plane_id((me + r) % PLANE),
                device_id_type=MESH,
            ).start()
            return carry

        lax.fori_loop(1, PLANE, spread, 0)
        arrived(recv3.at[pl.ds(0, PIECES - 1)], rsem3)
        arrived(recv1.at[pl.ds(0, PIECES - 1)], send1)
        arrived(recv2.at[pl.ds(0, NZ - 1)], send2)
        arrived(recv1.at[pl.ds(0, PLANE - 1)], send3)

    @pl.when(jnp.logical_not(owner))
    def _():
        arrived(recv3.at[pl.ds(0, PIECES)], rsem3)
        arrived(recv1.at[pl.ds(0, PIECES)], send1)

    @pl.when(has_left)
    def _():
        arrived(from_right, left_send)

    @pl.when(has_right)
    def _():
        arrived(from_left, right_send)

    store.wait()
    for i in range(PIECES):
        o_ref[pl.ds(8 * i, 8), :] = recv3[i]


def filter_and_reduce(states, diag_blocks, couplings):
    n = states.shape[0]
    tile = (128, 128)
    dma = pltpu.SemaphoreType.DMA
    return pl.pallas_call(
        filter_kernel,
        out_shape=(
            jax.ShapeDtypeStruct((n, 128), f32),
            jax.ShapeDtypeStruct((PIECES * 8, 128), f32),
        ),
        in_specs=[pl.BlockSpec(memory_space=pl.ANY)] * 3,
        out_specs=(pl.BlockSpec(memory_space=pl.ANY), pl.BlockSpec(memory_space=pltpu.VMEM)),
        scratch_shapes=[
            pltpu.VMEM((n, 128), f32),
            pltpu.VMEM((4,) + tile, f32),
            pltpu.VMEM((4,) + tile, f32),
            pltpu.VMEM((2,) + tile, f32),
            pltpu.VMEM((2,) + tile, f32),
            pltpu.VMEM((4,) + tile, f32),
            pltpu.VMEM((3,) + tile, f32),
            pltpu.VMEM((n, 128), f32),
            pltpu.VMEM((PIECES, 8, 128), f32),
            pltpu.VMEM((PLANE, 8, 128), f32),
            pltpu.VMEM((NZ, 8, 128), f32),
            pltpu.VMEM((PIECES, 8, 128), f32),
            dma((3,)), dma(()), dma(()), dma(()), dma((4,)), dma((3,)),
            dma(()), dma(()), dma(()), dma(()), dma(()), dma(()),
        ],
        compiler_params=pltpu.CompilerParams(collective_id=0, has_side_effects=True),
    )(states, diag_blocks, couplings)


def body(states, diag_blocks, couplings):
    total_nodes = states.shape[0] * lax.axis_size(DOM)
    flat, packed = filter_and_reduce(states, diag_blocks, couplings)
    return finish(packed, flat, total_nodes)


def solution(mesh):
    split = Mesh(mesh.devices.reshape(NZ, NX, NY, NC), DOM)
    in_specs = (P(DOM, None), P(DOM, None, None), P(DOM, None, None))
    out_specs = (P(DOM, None), P())
    return jax.shard_map(body, mesh=split, in_specs=in_specs, out_specs=out_specs, check_vma=False)
```

```python
import functools
import math

import jax
import jax.numpy as jnp
from jax import lax
from jax.experimental import pallas as pl
from jax.experimental.pallas import tpu as pltpu
from jax.sharding import Mesh
from jax.sharding import PartitionSpec as P

DOM = ("dom_0", "dom_1", "dom_2", "dom_3")
NZ, NX, NY, NC = 12, 4, 8, 2
PLANE = NX * NY * NC
PIECES = 17
ROWS = 4
GRANT = 8 * 1024 * 1024
MESH = pl.DeviceIdType.MESH

center = 0.5
half_width = 4.0

BS = 32
bf16 = jnp.bfloat16
f32 = jnp.float32


def split2(v):
    hi = v.astype(bf16)
    return hi, (v - hi.astype(f32)).astype(bf16)


def split3(v):
    hi = v.astype(bf16)
    rest = v - hi.astype(f32)
    mid = rest.astype(bf16)
    return hi, mid, (rest - mid.astype(f32)).astype(bf16)


def dot(a, b, ca=1, cb=0):
    return lax.dot_general(a, b, (((ca,), (cb,)), ((), ())), preferred_element_type=f32)


def dot6(a, b, ca=1, cb=0):
    (ah, am, al), (bh, bm, bl) = split3(a), split3(b)
    left = jnp.concatenate([ah, ah, am, am, ah, al], axis=ca)
    right = jnp.concatenate([bh, bm, bh, bm, bl, bh], axis=cb)
    return dot(left, right, ca, cb)


def dot3(a, b, ca=1, cb=0):
    (ah, al), (bh, bl) = split2(a), split2(b)
    return dot(ah, bh, ca, cb) + (dot(ah, bl, ca, cb) + dot(al, bh, ca, cb))


def spread_row(tile, s, width):
    return jnp.broadcast_to(tile[s : s + 1, :], (8, width))


def inverse_factor(a_ref, r_ref):
    n = 128
    tiles = BS // 8
    rows8 = lax.broadcasted_iota(jnp.int32, (8, 128), 0)
    for block in range(n // BS):
        base = block * BS
        square = a_ref[pl.ds(base, BS), :]
        cols = {}
        for j in range(BS):
            for r in range(j // 8, tiles):
                cols[j, r] = jnp.broadcast_to(
                    square[8 * r : 8 * r + 8, base + j : base + j + 1], (8, 128)
                )
        pa = [square[8 * r : 8 * r + 8, :] for r in range(tiles)]
        pr = [r_ref[pl.ds(base + 8 * r, 8), :] for r in range(tiles)]
        for k in range(BS):
            rk, sk = k // 8, k % 8
            inv = lax.rsqrt(spread_row(cols[k, rk], sk, 128))
            low = {r: cols[k, r] * inv for r in range(rk, tiles)}
            for j in range(k + 1, BS):
                factor = spread_row(low[j // 8], j % 8, 128)
                for r in range(j // 8, tiles):
                    cols[j, r] = cols[j, r] - low[r] * factor
            row_a = spread_row(pa[rk], sk, 128) * inv
            row_r = spread_row(pr[rk], sk, 128) * inv
            for r in range(rk, tiles):
                scale = low[r]
                if r == rk:
                    scale = jnp.where(rows8 > sk, scale, 0.0)
                na, nr = pa[r] - scale * row_a, pr[r] - scale * row_r
                if r == rk:
                    na, nr = jnp.where(rows8 == sk, row_a, na), jnp.where(rows8 == sk, row_r, nr)
                pa[r], pr[r] = na, nr
        upper = jnp.concatenate(pa, axis=0)
        below = jnp.concatenate(pr, axis=0)
        r_ref[pl.ds(base, BS), :] = below
        rest = n - base - BS
        if rest:
            both = jnp.concatenate([upper, below], axis=1)
            h, m, l = split3(both)
            lhs = jnp.concatenate([h, h, m, m, h, l], axis=0)[:, :128]
            rhs = jnp.concatenate([h, m, h, m, l, h], axis=0)
            update = dot(lhs, rhs, 0, 0)
            start = base + BS
            a_ref[pl.ds(start, rest), :] = a_ref[pl.ds(start, rest), :] - update[start:, :128]
            r_ref[pl.ds(start, rest), :] = r_ref[pl.ds(start, rest), :] - update[start:, 128:]


def finish_kernel(total_nodes, inv_ref, mixed_ref, f_ref, o_ref, p_ref):
    inv = inv_ref[...]
    p_ref[...] = dot6(dot6(inv, mixed_ref[...]), inv, 1, 1)
    o_ref[...] = dot3(f_ref[...], inv * math.sqrt(total_nodes), 1, 1)


def finish(inv, mixed, flat, total_nodes):
    n = flat.shape[0]
    return pl.pallas_call(
        functools.partial(finish_kernel, total_nodes),
        out_shape=(jax.ShapeDtypeStruct((n, 128), f32), jax.ShapeDtypeStruct((128, 128), f32)),
        in_specs=[pl.BlockSpec(memory_space=pltpu.VMEM)] * 3,
        out_specs=(pl.BlockSpec(memory_space=pltpu.VMEM),) * 2,
        compiler_params=pltpu.CompilerParams(vmem_limit_bytes=GRANT),
    )(inv, mixed, flat)


def halves(v):
    hi = v.astype(bf16)
    return hi, (v - hi.astype(f32)).astype(bf16)


def mul(a, b):
    (ah, al), (bh, bl) = a, b
    return dot(ah, bh) + (dot(ah, bl) + dot(al, bh))


def flip(pair):
    return tuple(part.T for part in pair)


def far(offset):
    return min(offset[0], NX - offset[0]) + min(offset[1], NY - offset[1])


CHIPS = sorted(((dx, dy) for dx in range(NX) for dy in range(NY)), key=far, reverse=True)
EVEN = [o for o in CHIPS if sum(o) % 2 == 0]
ODD = [o for o in CHIPS if sum(o) % 2 == 1]
RING = sorted(range(1, NZ), key=lambda r: min(r, NZ - r), reverse=True)


def fold(full):
    rows = lax.broadcasted_iota(jnp.int32, (64, 128), 0)
    lanes = lax.broadcasted_iota(jnp.int32, (64, 128), 1) - 64
    top, bottom = full[:64], full[64:]
    both = jnp.where(jnp.logical_and(lanes >= 0, rows >= lanes), pltpu.roll(top, 64, 1), bottom)
    diagonal = jnp.sum(jnp.where(rows == lanes, bottom, 0.0), axis=0, keepdims=True)
    return both, diagonal


def unfold(both, diagonal):
    rows = lax.broadcasted_iota(jnp.int32, (64, 128), 0)
    lanes = lax.broadcasted_iota(jnp.int32, (64, 128), 1)
    rolled = pltpu.roll(both, 64, 1)
    turned = jnp.concatenate([both, rolled], axis=0).T
    top = jnp.where(jnp.logical_and(lanes < 64, rows >= lanes), rolled, turned[64:])
    bottom = jnp.where(jnp.logical_and(lanes >= 64, rows >= lanes - 64), turned[:64], both)
    bottom = jnp.where(lanes - 64 == rows, jnp.broadcast_to(diagonal, (64, 128)), bottom)
    return jnp.concatenate([top, bottom], axis=0)


def filter_kernel(
    s_ref, d_ref, c_ref, f_ref, inv_ref, mixed_ref,
    s, d, cp, out_left, out_right, from_right, from_left, pieces, totals, recv1, recv2, a_ref,
    load_sem, left_send, right_send, right_sem, left_sem, send1, rsem1, send2, rsem2, send3, rsem3,
):
    z, x, y, c = (lax.axis_index(a) for a in DOM)
    me = (x * NY + y) * NC + c
    lin = z * PLANE + me
    has_left = lin > 0
    has_right = lin < NZ * PLANE - 1
    even = (x + y) % 2 == 0
    owner = jnp.logical_or(even, jnp.logical_and(x == 0, y == 1))
    mine = jnp.where(even, x * 4 + y // 2, 16)

    loads = [
        pltpu.make_async_copy(src, dst, load_sem.at[i])
        for i, (src, dst) in enumerate(((s_ref, s), (c_ref, cp), (d_ref, d)))
    ]
    for load in loads:
        load.start()

    def chain_id(t):
        return (t // PLANE, (t // (NY * NC)) % NX, (t // NC) % NY, t % NC)

    def shift(dx, dy, core):
        return (z, (x + dx) % NX, (y + dy) % NY, core)

    def to_even(k):
        dx = jnp.where(even, EVEN[k][0], ODD[k][0])
        dy = jnp.where(even, EVEN[k][1], ODD[k][1])
        return (x + dx) % NX, (y + dy) % NY

    barrier = pltpu.get_barrier_semaphore()

    def greet(target):
        pl.semaphore_signal(barrier, inc=1, device_id=target, device_id_type=MESH)

    @pl.when(has_left)
    def _():
        greet(chain_id(lin - 1))

    @pl.when(has_right)
    def _():
        greet(chain_id(lin + 1))

    @pl.when(owner)
    def _():
        for r in RING:
            greet(((z + r) % NZ, x, y, c))
        for dx, dy in CHIPS[:-1]:
            for core in range(NC):
                greet(shift(dx, dy, core))
        greet((z, x, y, 1 - c))

    @pl.when(jnp.logical_not(owner))
    def _():
        for core in range(NC):
            greet((z, 0, 1, core))
        for k in range(16):
            ox, oy = to_even(k)
            for core in range(NC):
                greet((z, ox, oy, core))

    def arrived(ref, sem):
        pltpu.make_async_copy(ref, ref, sem).wait()

    def send(src, dst, send_sem, recv_sem, target):
        pltpu.make_async_remote_copy(
            src_ref=src, dst_ref=dst, send_sem=send_sem, recv_sem=recv_sem,
            device_id=target, device_id_type=MESH,
        ).start()

    rows = lax.broadcasted_iota(jnp.int32, (128, 128), 0)
    cols = lax.broadcasted_iota(jnp.int32, (128, 128), 1)
    eye = rows == cols

    def shifted(raw):
        return halves(0.5 * (raw + raw.T) - jnp.where(eye, center, 0.0))

    quarter, half = 1.0 / half_width, 2.0 / half_width
    loads[0].wait()
    loads[1].wait()
    sv = [s[pl.ds(128 * b, 128), :] for b in range(4)]
    ss = [halves(v) for v in sv]
    cc = [halves(cp[b]) for b in range(4)]
    ct = [flip(v) for v in cc]
    u = mul(ct[3], ss[3]) * quarter
    out_right[0] = u
    loads[2].wait()
    aa = [shifted(d[b]) for b in range(4)]
    p0 = (mul(aa[0], ss[0]) + mul(cc[0], ss[1])) * quarter
    out_left[0] = p0
    h3 = (mul(aa[3], ss[3]) + mul(ct[2], ss[2])) * quarter
    h3s = halves(h3)
    w = mul(ct[3], h3s) * half
    out_right[1] = w

    greeted = has_left.astype(jnp.int32) + has_right.astype(jnp.int32)
    pl.semaphore_wait(barrier, jnp.where(owner, PLANE - 1 + NZ - 1, 2 * PIECES) + greeted)

    @pl.when(has_right)
    def _():
        for i, src in enumerate((cp.at[3], out_right.at[0], out_right.at[1])):
            send(src, from_left.at[i], right_send, left_sem.at[i], chain_id(lin + 1))

    @pl.when(has_left)
    def _():
        for i, src in enumerate((s.at[pl.ds(0, 128)], out_left.at[0], d.at[0])):
            send(src, from_right.at[i], left_send, right_sem.at[i], chain_id(lin - 1))

    @pl.when(jnp.logical_not(has_right))
    def _():
        from_right[...] = jnp.zeros_like(from_right)

    @pl.when(jnp.logical_not(has_left))
    def _():
        from_left[...] = jnp.zeros_like(from_left)

    p0s, us = halves(p0), halves(u)
    g1 = (mul(aa[1], ss[1]) + mul(cc[1], ss[2]) + mul(ct[0], ss[0])) * quarter
    g1s = halves(g1)
    q0 = (mul(aa[0], p0s) + mul(cc[0], g1s)) * half - sv[0]
    out_left[1] = q0

    @pl.when(has_left)
    def _():
        send(out_left.at[1], from_right.at[3], left_send, right_sem.at[3], chain_id(lin - 1))

    g2 = (mul(aa[2], ss[2]) + mul(cc[2], ss[3]) + mul(ct[1], ss[1])) * quarter
    g2s = halves(g2)
    e1 = (mul(aa[1], g1s) + mul(ct[0], p0s) + mul(cc[1], g2s)) * half - sv[1]
    e2 = (mul(aa[2], g2s) + mul(ct[1], g1s) + mul(cc[2], h3s)) * half - sv[2]
    e3 = (mul(aa[3], h3s) + mul(ct[2], g2s)) * half - sv[3]

    @pl.when(has_right)
    def _():
        arrived(from_right.at[0], right_sem.at[0])
        arrived(from_right.at[1], right_sem.at[1])

    inside = jnp.where(has_right, 1.0, 0.0)
    vs = halves(mul(cc[3], halves(from_right[0])) * quarter)
    g3s = halves(h3 + mul(cc[3], halves(from_right[0])) * quarter)
    g4s = halves((from_right[1] + u) * inside)
    f2 = e2 + mul(cc[2], vs) * half
    f3 = e3 + (mul(aa[3], vs) + mul(cc[3], g4s)) * half

    @pl.when(has_left)
    def _():
        for i in range(3):
            arrived(from_left.at[i], left_sem.at[i])

    cl = halves(from_left[0])
    ul = halves(from_left[1])
    f1 = e1 + mul(ct[0], ul) * half
    back = mul(flip(cl), halves(mul(cl, ss[0])))
    f0 = q0 + mul(aa[0], ul) * half + from_left[2] + back * (half * quarter)
    fs = [f0, f1, f2, f3]
    for b in range(4):
        f_ref[pl.ds(128 * b, 128), :] = fs[b]
    fh = [halves(f) for f in fs]

    def stack(pairs):
        return tuple(jnp.concatenate(parts, axis=0) for parts in zip(*pairs))

    turned = flip(stack(fh))

    def deal(kind, full):
        both, diagonal = fold(full)
        for i in range(16):
            pieces[kind, i] = both[ROWS * i : ROWS * i + ROWS, :]
        pieces[kind, 16] = jnp.broadcast_to(diagonal, (ROWS, 128))
        core = 1 - kind

        def out(piece, ox, oy):
            target = (ox * NY + oy) * NC + core
            send(
                pieces.at[kind, piece], recv1.at[(me - target + PLANE) % PLANE], send1, rsem1,
                (z, ox, oy, core),
            )

        @pl.when(me != NC + core)
        def _():
            out(16, 0, 1)

        for k in range(15):
            ox, oy = to_even(k)
            out(ox * 4 + oy // 2, ox, oy)
        ox, oy = to_even(15)

        @pl.when(jnp.logical_and(owner, c == core))
        def _():
            recv1[0] = pieces[kind, mine]

        @pl.when((ox * NY + oy) * NC + core != me)
        def _():
            out(ox * 4 + oy // 2, ox, oy)

    deal(0, mul(turned, stack(fh)))

    @pl.when(has_right)
    def _():
        arrived(from_right.at[2], right_sem.at[2])
        arrived(from_right.at[3], right_sem.at[3])

    f4 = (from_right[3] + (mul(shifted(from_right[2]), us) + mul(ct[3], g3s)) * half) * inside
    fh = fh + [halves(f4)]
    part = [mul(halves(0.5 * d[b]), fh[b]) + mul(cc[b], fh[b + 1]) for b in range(4)]
    cross = mul(turned, stack([halves(g) for g in part]))
    deal(1, cross + cross.T)

    @pl.when(owner)
    def _():
        kind = 1 - c
        arrived(recv1.at[pl.ds(1, PLANE - 1)], rsem1)
        recv2[z] = jnp.sum(recv1[...], axis=0)
        for r in RING:
            send(recv2.at[z], recv2.at[z], send2, rsem2, ((z + r) % NZ, x, y, c))
        arrived(recv2.at[pl.ds(0, NZ - 1)], rsem2)
        totals[kind, mine] = jnp.sum(recv2[...], axis=0)
        ours = totals.at[kind, mine]
        for dx, dy in CHIPS[:-1]:
            for core in range(NC):
                send(ours, ours, send3, rsem3.at[kind], shift(dx, dy, core))
        send(ours, ours, send3, rsem3.at[kind], (z, x, y, 1 - c))

    def collect(kind):
        holder = jnp.logical_and(owner, c == 1 - kind)

        @pl.when(holder)
        def _():
            arrived(totals.at[kind, pl.ds(0, PIECES - 1)], rsem3.at[kind])

        @pl.when(jnp.logical_not(holder))
        def _():
            arrived(totals.at[kind], rsem3.at[kind])

        both = jnp.concatenate([totals[kind, i] for i in range(16)], axis=0)
        return unfold(both, totals[kind, 16][:1])

    a_ref[...] = collect(0)
    inv_ref[...] = jnp.where(eye, 1.0, 0.0)
    inverse_factor(a_ref, inv_ref)
    mixed_ref[...] = collect(1)

    @pl.when(owner)
    def _():
        arrived(recv2.at[pl.ds(0, NZ - 1)], send2)
        arrived(recv1.at[pl.ds(0, PLANE - 1)], send3)
        arrived(recv1.at[pl.ds(0, 2 * PIECES - 1)], send1)

    @pl.when(jnp.logical_not(owner))
    def _():
        arrived(recv1.at[pl.ds(0, 2 * PIECES)], send1)

    @pl.when(has_left)
    def _():
        arrived(from_right, left_send)

    @pl.when(has_right)
    def _():
        arrived(from_left, right_send)


def filter_and_reduce(states, diag_blocks, couplings):
    n = states.shape[0]
    tile = (128, 128)
    dma = pltpu.SemaphoreType.DMA
    return pl.pallas_call(
        filter_kernel,
        out_shape=(
            jax.ShapeDtypeStruct((n, 128), f32),
            jax.ShapeDtypeStruct(tile, f32),
            jax.ShapeDtypeStruct(tile, f32),
        ),
        in_specs=[pl.BlockSpec(memory_space=pltpu.HBM)] * 3,
        out_specs=(pl.BlockSpec(memory_space=pltpu.VMEM),) * 3,
        scratch_shapes=[
            pltpu.VMEM((n, 128), f32),
            pltpu.VMEM((4,) + tile, f32),
            pltpu.VMEM((4,) + tile, f32),
            pltpu.VMEM((2,) + tile, f32),
            pltpu.VMEM((2,) + tile, f32),
            pltpu.VMEM((4,) + tile, f32),
            pltpu.VMEM((3,) + tile, f32),
            pltpu.VMEM((2, PIECES, ROWS, 128), f32),
            pltpu.VMEM((2, PIECES, ROWS, 128), f32),
            pltpu.VMEM((PLANE, ROWS, 128), f32),
            pltpu.VMEM((NZ, ROWS, 128), f32),
            pltpu.VMEM(tile, f32),
            dma((3,)), dma(()), dma(()), dma((4,)), dma((3,)),
            dma(()), dma(()), dma(()), dma(()), dma(()), dma((2,)),
        ],
        compiler_params=pltpu.CompilerParams(
            collective_id=0, has_side_effects=True, vmem_limit_bytes=GRANT
        ),
    )(*(pltpu.with_memory_space_constraint(v, pltpu.HBM) for v in (states, diag_blocks, couplings)))


def body(states, diag_blocks, couplings):
    total_nodes = states.shape[0] * lax.axis_size(DOM)
    flat, inv, mixed = filter_and_reduce(states, diag_blocks, couplings)
    return finish(inv, mixed, flat, total_nodes)


def solution(mesh):
    split = Mesh(mesh.devices.reshape(NZ, NX, NY, NC), DOM)
    in_specs = (P(DOM, None), P(DOM, None, None), P(DOM, None, None))
    out_specs = (P(DOM, None), P())
    return jax.shard_map(body, mesh=split, in_specs=in_specs, out_specs=out_specs, check_vma=False)
```
